128 devices in a mesh: replica: 1, heads: 64 (over z, y, x), model: 2 (over core).
Axes of the slice: x: 4, y: 4, z: 4, core: 2. Of those that a mesh axis runs over, the one named last changes fastest.
Arguments:
- tokens: bfloat16 [32, 16384], P('replica')
- w_query: bfloat16 [16384, 16384], P(None, ('heads', 'model'))
- w_key: bfloat16 [16384, 1024], replicated
- w_value: bfloat16 [16384, 1024], replicated
- w_out: bfloat16 [16384, 16384], P(('heads', 'model'))
- key_cache: bfloat16 [32, 8, 2048, 128], P(('replica', 'model'))
- value_cache: bfloat16 [32, 8, 2048, 128], P(('replica', 'model'))
- lengths: int32 [32], P(('replica', 'model'))
Outputs:
- output 1: bfloat16 [32, 16384], P('replica')
- output 2: bfloat16 [32, 8, 128], P(('replica', 'model'))
- output 3: bfloat16 [32, 8, 128], P(('replica', 'model'))
All inputs are finite; a program needn't handle non-finite values.
Results may differ from the reference program's by a relative error of at most 0.00215798.
Values are sent between devices in bfloat16 or wider.
A program may use at most 1 GiB of HBM per device.

```python
import jax
import jax.numpy as jnp
from jax import lax

D = 16384
QHEADS = 128
KVHEADS = 8
HEAD = 128
BATCH = 32
CONTEXT = 2048
GROUP_SIZE = QHEADS // KVHEADS
SCALE = HEAD ** -0.5


def draw_lengths(len_key):
    len_keys = jax.random.split(len_key, 2)
    lengths = jax.random.randint(len_keys[0], (BATCH,), 1, CONTEXT, dtype=jnp.int32)
    perm_order = jax.random.permutation(len_keys[1], BATCH)
    return lengths.at[perm_order[0]].set(CONTEXT - 1).at[perm_order[1]].set(1)


def setup_inputs(seed: int = 0, part: int = 0) -> dict:
    base_key = jax.random.key(seed)
    part_key = jax.random.fold_in(base_key, part)
    part_keys = jax.random.split(part_key, 3)
    weight_keys = jax.random.split(base_key, 4)
    query_cols = QHEADS * HEAD
    kv_cols = KVHEADS * HEAD
    tokens = jax.random.normal(part_keys[0], (BATCH, D), jnp.float32)
    w_query = jax.random.normal(weight_keys[0], (D, query_cols), jnp.float32) * D ** -0.5
    w_key = jax.random.normal(weight_keys[1], (D, kv_cols), jnp.float32) * (3.0 * D ** -0.5)
    w_value = jax.random.normal(weight_keys[2], (D, kv_cols), jnp.float32) * D ** -0.5
    w_out = jax.random.normal(weight_keys[3], (query_cols, D), jnp.float32) * query_cols ** -0.5
    key_cache = 3.0 * jax.random.normal(part_keys[1], (BATCH, KVHEADS, CONTEXT, HEAD), jnp.float32)
    value_cache = jax.random.normal(part_keys[2], (BATCH, KVHEADS, CONTEXT, HEAD), jnp.float32)
    lengths = draw_lengths(jax.random.fold_in(part_key, 3))
    return {
        "tokens": tokens.astype(jnp.bfloat16),
        "w_query": w_query.astype(jnp.bfloat16),
        "w_key": w_key.astype(jnp.bfloat16),
        "w_value": w_value.astype(jnp.bfloat16),
        "w_out": w_out.astype(jnp.bfloat16),
        "key_cache": key_cache.astype(jnp.bfloat16),
        "value_cache": value_cache.astype(jnp.bfloat16),
        "lengths": lengths,
    }


def reference(tokens, w_query, w_key, w_value, w_out, key_cache, value_cache, lengths):
    queries = jnp.dot(tokens, w_query, preferred_element_type=jnp.float32).astype(jnp.bfloat16)
    queries = queries.reshape(BATCH, KVHEADS, GROUP_SIZE, HEAD)
    key_new = jnp.dot(tokens, w_key, preferred_element_type=jnp.float32).astype(jnp.bfloat16)
    key_new = key_new.reshape(BATCH, KVHEADS, HEAD)
    value_new = jnp.dot(tokens, w_value, preferred_element_type=jnp.float32).astype(jnp.bfloat16)
    value_new = value_new.reshape(BATCH, KVHEADS, HEAD)

    def one_sequence(item):
        q_seq, key_seq, value_seq, key_last, value_last, seq_len = item
        q_wide = q_seq.astype(jnp.float32)
        scores = jnp.einsum("grd,gtd->grt", q_wide, key_seq.astype(jnp.float32)) * SCALE
        score_new = jnp.einsum("grd,gd->gr", q_wide, key_last.astype(jnp.float32)) * SCALE
        positions = jnp.arange(CONTEXT)
        scores = jnp.where(positions < seq_len, scores, -jnp.inf)
        score_max = jnp.maximum(jnp.max(scores, axis=-1), score_new)
        weights = jnp.exp(scores - score_max[..., None])
        weight_new = jnp.exp(score_new - score_max)
        denom_sum = jnp.sum(weights, axis=-1) + weight_new
        weighted_sum = jnp.einsum("grt,gtd->grd", weights.astype(jnp.bfloat16).astype(jnp.float32), value_seq.astype(jnp.float32))
        weighted_sum = weighted_sum + weight_new.astype(jnp.bfloat16).astype(jnp.float32)[..., None] * value_last.astype(jnp.float32)[:, None, :]
        return (weighted_sum / denom_sum[..., None]).astype(jnp.bfloat16)

    attended = lax.map(one_sequence, (queries, key_cache, value_cache, key_new, value_new, lengths))
    mixed_sum = jnp.dot(attended.reshape(BATCH, QHEADS * HEAD), w_out, preferred_element_type=jnp.float32)
    out_tokens = (tokens.astype(jnp.float32) + mixed_sum).astype(jnp.bfloat16)
    return (out_tokens, key_new, value_new)
```

```python
import functools

import jax
import jax.numpy as jnp
from jax import lax
from jax.experimental import pallas as pl
from jax.experimental.pallas import tpu as pltpu
from jax.sharding import PartitionSpec as P

MESH = pl.DeviceIdType.MESH
ROTATIONS = ((0, 1, 2), (1, 2, 0), (2, 0, 1))


def attend(queries, key_rows, value_rows, key_last, value_last, seq_len):
    score_scale = queries.shape[-1] ** -0.5
    scores = jnp.einsum("bgrd,bgtd->bgrt", queries, key_rows, preferred_element_type=jnp.float32) * score_scale
    score_new = jnp.einsum("bgrd,bgd->bgr", queries, key_last, preferred_element_type=jnp.float32) * score_scale
    positions = lax.broadcasted_iota(jnp.int32, (1, 1, 1, key_rows.shape[2]), 3)
    scores = jnp.where(positions < seq_len[:, None, None, None], scores, -jnp.inf)
    score_max = jnp.maximum(jnp.max(scores, axis=-1), score_new)
    weights = jnp.exp(scores - score_max[..., None])
    weight_new = jnp.exp(score_new - score_max)
    denom_sum = jnp.sum(weights, axis=-1) + weight_new
    weighted_sum = jnp.einsum("bgrt,bgtd->bgrd", weights.astype(jnp.bfloat16), value_rows, preferred_element_type=jnp.float32)
    weighted_sum = weighted_sum + weight_new.astype(jnp.bfloat16).astype(jnp.float32)[..., None] * value_last.astype(jnp.float32)[:, :, None, :]
    return (weighted_sum / denom_sum[..., None]).astype(jnp.bfloat16)


def pick(rot, values):
    if isinstance(rot, int):
        return values[rot]
    return jnp.where(rot == 0, values[0], jnp.where(rot == 1, values[1], values[2]))


def peer_along(rot, place, coord, step):
    out = []
    for dims in ROTATIONS:
        dim = dims[place]
        moved = [coord[0], coord[1], coord[2]]
        moved[dim] = lax.rem(coord[dim] + step, 4)
        out.append((moved[2] * 4 + moved[1]) * 4 + moved[0])
    return pick(rot, out)


def coord_along(rot, place, coord):
    return pick(rot, [coord[dims[place]] for dims in ROTATIONS])


def mix_kernel(o_ref, w_ref, tok_ref, out_ref, wbuf, part, r1, acc1, r2, acc2, r3, fin, tokbuf, agbuf,
               wsem, wsend, wrecv, s1, v1, s2, v2, s3, v3, ag_s, ag_v, dd_s, dd_v):
    core = lax.axis_index("model")
    chip = lax.axis_index("heads")
    coord = (lax.rem(chip, 4), lax.rem(lax.div(chip, 4), 4), lax.div(chip, 16))
    half = 8192
    my_col = pl.multiple_of(core * half, half)
    other_col = pl.multiple_of((1 - core) * half, half)
    my_row = pl.multiple_of(core * 128, 128)

    w_local = pltpu.make_async_copy(w_ref.at[:, pl.ds(my_col, half)], wbuf.at[pl.ds(my_row, 128)], wsem.at[0])
    w_local.start()
    t_local = pltpu.make_async_copy(
        tok_ref.at[:, pl.ds(pl.multiple_of(core * half + chip * 128, 128), 128)], tokbuf, wsem.at[1])
    t_local.start()

    barrier = pltpu.get_barrier_semaphore()
    pl.semaphore_signal(barrier, inc=1, device_id={"heads": chip, "model": 1 - core}, device_id_type=MESH)
    for place in range(3):
        for k in (1, 2, 3):
            pl.semaphore_signal(
                barrier, inc=1, device_id={"heads": peer_along(0, place, coord, k), "model": core}, device_id_type=MESH)
    pl.semaphore_wait(barrier, 10)

    w_remote = pltpu.make_async_remote_copy(
        src_ref=w_ref.at[:, pl.ds(other_col, half)], dst_ref=wbuf.at[pl.ds(my_row, 128)],
        send_sem=wsend, recv_sem=wrecv, device_id={"heads": chip, "model": 1 - core}, device_id_type=MESH)
    w_remote.start()

    rots = (0, 1, 2, core)
    w_local.wait()
    w_remote.wait_recv()
    o = o_ref[...]

    @pl.loop(0, 16)
    def _(t):
        bz, by = lax.div(t, 4), lax.rem(t, 4)
        res = jnp.dot(o, wbuf[:, pl.ds(pl.multiple_of(t * 512, 512), 512)], preferred_element_type=jnp.float32)
        for bx in range(4):
            block = (bx, by, bz)
            for rg in range(4):
                at = pick(rots[rg], [block[d[0]] * 16 + block[d[1]] * 4 + block[d[2]] for d in ROTATIONS])
                part[rg, at] = res[rg * 8:rg * 8 + 8, bx * 128:bx * 128 + 128]

    def exchange(rg, place, src, width, dst, ssem, rsem):
        copies = []
        mine = coord_along(rots[rg], place, coord)
        for k in (1, 2, 3):
            there = lax.rem(mine + k, 4)
            copy = pltpu.make_async_remote_copy(
                src_ref=src.at[rg, pl.ds(there * width, width)], dst_ref=dst.at[rg, k - 1],
                send_sem=ssem.at[rg, k - 1], recv_sem=rsem.at[rg, k - 1],
                device_id={"heads": peer_along(rots[rg], place, coord, k), "model": core}, device_id_type=MESH)
            copy.start()
            copies.append(copy)
        return copies

    def collect(rg, place, src, width, dst, copies):
        for copy in copies:
            copy.wait_recv()
        mine = coord_along(rots[rg], place, coord)
        return src[rg, pl.ds(mine * width, width)] + dst[rg, 0] + dst[rg, 1] + dst[rg, 2]

    sent = []
    c1 = [exchange(rg, 0, part, 16, r1, s1, v1) for rg in range(4)]
    c2 = []
    for rg in range(4):
        acc1[rg] = collect(rg, 0, part, 16, r1, c1[rg])
        c2.append(exchange(rg, 1, acc1, 4, r2, s2, v2))
    c3 = []
    for rg in range(4):
        acc2[rg] = collect(rg, 1, acc1, 4, r2, c2[rg])
        c3.append(exchange(rg, 2, acc2, 1, r3, s3, v3))
    for rg in range(4):
        fin[pl.ds(rg * 8, 8)] = collect(rg, 2, acc2, 1, r3, c3[rg])[0]
    for group in (c1, c2, c3):
        for copies in group:
            sent += copies
    t_local.wait()
    block = (tokbuf[...].astype(jnp.float32) + fin[...]).astype(jnp.bfloat16)

    def ag_rot(cc, h):
        return (cc * 2 + h) % 3 if isinstance(cc, int) else (h if h == 0 else None)

    halves = []
    for h in range(2):
        rot = jnp.where(core == 0, ag_rot(0, h), ag_rot(1, h))
        a, b, c = (coord_along(rot, i, coord) for i in range(3))
        halves.append((rot, a, b, c))
        agbuf[core, h, c * 16 + b * 4 + a] = block[h * 16:h * 16 + 16]

    def spread(h, place, start, width):
        rot = halves[h][0]
        copies = []
        for k in (1, 2, 3):
            ref = agbuf.at[core, h, pl.ds(start, width)]
            copy = pltpu.make_async_remote_copy(
                src_ref=ref, dst_ref=ref, send_sem=ag_s.at[h, place, k - 1], recv_sem=ag_v.at[h, place, k - 1],
                device_id={"heads": peer_along(rot, place, coord, k), "model": core}, device_id_type=MESH)
            copy.start()
            copies.append(copy)
        return copies

    def across(h, k, start):
        ref = agbuf.at[core, h, pl.ds(start, 16)]
        copy = pltpu.make_async_remote_copy(
            src_ref=ref, dst_ref=ref, send_sem=dd_s.at[h, k], recv_sem=dd_v.at[h, k],
            device_id={"heads": chip, "model": 1 - core}, device_id_type=MESH)
        copy.start()
        return copy

    def arrive(h, place, k, width, base, stride, copy):
        copy.wait_recv()

    ga = [spread(h, 0, halves[h][3] * 16 + halves[h][2] * 4 + halves[h][1], 1) for h in range(2)]
    gb = []
    for h in range(2):
        for copy in ga[h]:
            copy.wait_recv()
        gb.append(spread(h, 1, halves[h][3] * 16 + halves[h][2] * 4, 4))
    gc, gd = [], []
    for h in range(2):
        for copy in gb[h]:
            copy.wait_recv()
        gc.append(spread(h, 2, halves[h][3] * 16, 16))
        gd.append([across(h, 0, halves[h][3] * 16)])
    for k in (1, 3, 2):
        for h in range(2):
            gc[h][k - 1].wait_recv()
            gd[h].append(across(h, k, lax.rem(halves[h][3] + 4 - k, 4) * 16))
    for h in range(2):
        for copy in gd[h]:
            copy.wait_recv()
    for cc in range(2):
        for h in range(2):
            dims = ROTATIONS[ag_rot(cc, h)]
            for bz in range(4):
                for by in range(4):
                    for bx in range(4):
                        b = (bx, by, bz)
                        at = b[dims[2]] * 16 + b[dims[1]] * 4 + b[dims[0]]
                        col = cc * half + ((bz * 4 + by) * 4 + bx) * 128
                        out_ref[h * 16:h * 16 + 16, col:col + 128] = agbuf[cc, h, at]
    w_remote.wait_send()
    for copies in (*ga, *gb, *gc, *gd, sent):
        for copy in copies:
            copy.wait_send()


def mix(o, w_out, tokens):
    f32, bf16 = jnp.float32, jnp.bfloat16
    dma = pltpu.SemaphoreType.DMA
    return pl.pallas_call(
        mix_kernel,
        out_shape=jax.ShapeDtypeStruct((32, 16384), bf16),
        in_specs=[pl.BlockSpec(memory_space=pltpu.VMEM), pl.BlockSpec(memory_space=pl.ANY), pl.BlockSpec(memory_space=pl.ANY)],
        out_specs=pl.BlockSpec(memory_space=pltpu.VMEM),
        scratch_shapes=[
            pltpu.VMEM((256, 8192), bf16), pltpu.VMEM((4, 64, 8, 128), f32), pltpu.VMEM((4, 3, 16, 8, 128), f32),
            pltpu.VMEM((4, 16, 8, 128), f32), pltpu.VMEM((4, 3, 4, 8, 128), f32), pltpu.VMEM((4, 4, 8, 128), f32),
            pltpu.VMEM((4, 3, 1, 8, 128), f32), pltpu.VMEM((32, 128), f32), pltpu.VMEM((32, 128), bf16),
            pltpu.VMEM((2, 2, 64, 16, 128), bf16),
            dma((2,)), dma, dma, dma((4, 3)), dma((4, 3)), dma((4, 3)), dma((4, 3)), dma((4, 3)), dma((4, 3)),
            dma((2, 3, 3)), dma((2, 3, 3)), dma((2, 4)), dma((2, 4)),
        ],
        compiler_params=pltpu.CompilerParams(collective_id=0, has_side_effects=True),
    )(o, w_out, tokens)


def solution(mesh):
    heads_count = mesh.shape["heads"]
    model_count = mesh.shape["model"]

    def local_step(tokens, w_query, w_key, w_value, w_out, key_cache, value_cache, lengths):
        batch_all = tokens.shape[0]
        local_rows = key_cache.shape[0]
        kv_count = key_cache.shape[1]
        head_dim = key_cache.shape[3]
        heads_local = w_query.shape[1] // head_dim
        heads_shard = heads_local * model_count
        group_size = heads_shard * heads_count // kv_count
        shard_groups = max(1, heads_shard // group_size)
        head_index = lax.axis_index("heads")
        model_index = lax.axis_index("model")
        queries = jnp.dot(tokens, w_query, preferred_element_type=jnp.float32).astype(jnp.bfloat16)
        queries = lax.all_to_all(queries.reshape(batch_all, heads_local, head_dim), "model", 0, 1, tiled=True)
        own_tokens = lax.dynamic_slice_in_dim(tokens, model_index * local_rows, local_rows, 0)
        key_new = jnp.dot(own_tokens, w_key, preferred_element_type=jnp.float32).astype(jnp.bfloat16)
        key_new = key_new.reshape(local_rows, kv_count, head_dim)
        value_new = jnp.dot(own_tokens, w_value, preferred_element_type=jnp.float32).astype(jnp.bfloat16)
        value_new = value_new.reshape(local_rows, kv_count, head_dim)
        first_group = head_index * heads_shard // group_size
        attended = attend(
            queries.reshape(local_rows, shard_groups, heads_shard // shard_groups, head_dim),
            lax.dynamic_slice_in_dim(key_cache, first_group, shard_groups, 1),
            lax.dynamic_slice_in_dim(value_cache, first_group, shard_groups, 1),
            lax.dynamic_slice_in_dim(key_new, first_group, shard_groups, 1),
            lax.dynamic_slice_in_dim(value_new, first_group, shard_groups, 1),
            lengths,
        )
        attended = lax.all_gather(attended.reshape(local_rows, heads_shard * head_dim), "model", axis=0, tiled=True)
        out_tokens = mix(attended, w_out, tokens)
        return (out_tokens, key_new, value_new)

    cache_spec = P(("replica", "model"), None, None, None)
    new_spec = P(("replica", "model"), None, None)
    return jax.shard_map(
        local_step,
        mesh=mesh,
        in_specs=(P("replica", None), P(None, ("heads", "model")), P(None, None), P(None, None), P(("heads", "model"), None), cache_spec, cache_spec, P(("replica", "model"))),
        out_specs=(P("replica", None), new_spec, new_spec),
        check_vma=False,
    )
```

```python
import jax
import jax.numpy as jnp
from jax import lax
from jax.experimental import pallas as pl
from jax.experimental.pallas import tpu as pltpu
from jax.sharding import PartitionSpec as P

MESH = pl.DeviceIdType.MESH
F32, BF16 = jnp.float32, jnp.bfloat16
ROTATIONS = ((0, 1, 2), (1, 2, 0), (2, 0, 1))
REDUCE_ROT = ((0, 1, 1, 2), (2, 0, 0, 1))
GATHER_ROT = ((0, 1), (2, 0))
BATCH_GROUPS = ((0, 2), (1, 3))
HALF = 8192
SCALE = 128 ** -0.5


def pick(rot, values):
    return jnp.where(rot == 0, values[0], jnp.where(rot == 1, values[1], values[2]))


def chip_of(coord):
    return (coord[2] * 4 + coord[1]) * 4 + coord[0]


def moved(coord, dim, step):
    out = list(coord)
    out[dim] = lax.rem(coord[dim] + step, 4)
    return out


def peer_along(rot, place, coord, step):
    return pick(rot, [chip_of(moved(coord, dims[place], step)) for dims in ROTATIONS])


def coord_along(rot, place, coord):
    return pick(rot, [coord[dims[place]] for dims in ROTATIONS])


def step_kernel(len_ref, tok_hbm, wq_hbm, wk_hbm, wv_hbm, wo_hbm, kc_hbm, vc_hbm, out_ref, new_ref,
                tok, wq, wkv, kbuf, vbuf, wbuf, qpair, qh, kvpair, nkv, kg, obuf, sbuf,
                part, r1, acc1, r2, acc2, r3, agbuf,
                tok_sem, wq_sem, wkv_sem, k_sem, v_sem, wo_sem, wos, wov, q_s, q_v, n_s, n_v, g_s, g_v, o_s, o_v,
                s1, v1, s2, v2, s3, v3, ag_s, ag_v, dd_s, dd_v):
    core = lax.axis_index("model")
    chip = lax.axis_index("heads")
    coord = (lax.rem(chip, 4), lax.rem(lax.div(chip, 4), 4), lax.div(chip, 16))
    group = lax.div(chip, 8)
    partner = {"heads": chip, "model": 1 - core}
    my_col = pl.multiple_of(core * HALF, HALF)
    other_col = pl.multiple_of((1 - core) * HALF, HALF)
    my_row = pl.multiple_of(core * 128, 128)
    kv_col = pl.multiple_of(group * 128, 128)

    tok_copy = pltpu.make_async_copy(tok_hbm, tok, tok_sem)
    wq_copies = [pltpu.make_async_copy(wq_hbm.at[pl.ds(i * 2048, 2048)], wq.at[i], wq_sem.at[i]) for i in range(8)]
    wk_copies = [pltpu.make_async_copy(wk_hbm.at[pl.ds(i * 2048, 2048), pl.ds(kv_col, 128)], wkv.at[i], wkv_sem.at[i]) for i in range(8)]
    wv_copies = [pltpu.make_async_copy(wv_hbm.at[pl.ds(i * 2048, 2048), pl.ds(kv_col, 128)], wkv.at[i], wkv_sem.at[i]) for i in range(8)]
    k_copies = [[pltpu.make_async_copy(kc_hbm.at[i * 8 + b, group], kbuf.at[i, :, pl.ds(b * 128, 128)], k_sem.at[i, b]) for b in range(8)] for i in range(2)]
    v_copies = [[pltpu.make_async_copy(vc_hbm.at[i * 8 + b, group], vbuf.at[i, :, pl.ds(b * 128, 128)], v_sem.at[i, b]) for b in range(8)] for i in range(2)]
    wo_copy = pltpu.make_async_copy(wo_hbm.at[:, pl.ds(my_col, HALF)], wbuf.at[pl.ds(my_row, 128)], wo_sem)

    def start_wkv(i):
        @pl.when(core == 0)
        def _():
            wk_copies[i].start()

        @pl.when(core == 1)
        def _():
            wv_copies[i].start()

    tok_copy.start()
    for i in range(8):
        wq_copies[i].start()

    barrier = pltpu.get_barrier_semaphore()
    pl.semaphore_signal(barrier, inc=1, device_id=partner, device_id_type=MESH)
    for dim in range(3):
        for k in (1, 2, 3):
            pl.semaphore_signal(
                barrier, inc=1, device_id={"heads": chip_of(moved(coord, dim, k)), "model": core}, device_id_type=MESH)
    for k in (1, 2, 3):
        pl.semaphore_signal(
            barrier, inc=1, device_id={"heads": chip_of(moved(moved(coord, 1, 2), 2, k)), "model": core}, device_id_type=MESH)

    tok_copy.wait()
    q_sum = jnp.zeros((32, 128), F32)
    for i in range(8):
        wq_copies[i].wait()
        start_wkv(i)
        q_sum += jnp.dot(tok[:, i * 2048:i * 2048 + 2048], wq[i], preferred_element_type=F32)
    q_new = q_sum.astype(BF16)
    qpair[0] = q_new[0:16]
    qpair[1] = q_new[16:32]
    qh[core] = qpair[core]
    pl.semaphore_wait(barrier, 13)

    def to_partner(src, dst, ssem, rsem):
        copy = pltpu.make_async_remote_copy(
            src_ref=src, dst_ref=dst, send_sem=ssem, recv_sem=rsem, device_id=partner, device_id_type=MESH)
        copy.start()
        return copy

    def wo_part(i):
        return to_partner(
            wo_hbm.at[:, pl.ds(pl.multiple_of(other_col + i * 4096, 4096), 4096)],
            wbuf.at[pl.ds(my_row, 128), pl.ds(i * 4096, 4096)],
            wos.at[i], wov.at[i])

    tail = []
    q_copy = to_partner(qpair.at[1 - core], qh.at[core], q_s, q_v)
    wo_remote = [wo_part(0)]

    kv_sum = jnp.zeros((32, 128), F32)
    for i in range(8):
        wk_copies[i].wait()
        k_copies[0][i].start()
        v_copies[0][i].start()
        kv_sum += jnp.dot(tok[:, i * 2048:i * 2048 + 2048], wkv[i], preferred_element_type=F32)
    kv_new = kv_sum.astype(BF16)
    kvpair[0] = kv_new[0:16]
    kvpair[1] = kv_new[16:32]
    nkv[core] = kvpair[core]
    n_copy = to_partner(kvpair.at[1 - core], nkv.at[core], n_s, n_v)
    wo_remote.append(wo_part(1))
    wo_copy.start()
    tail += [q_copy, n_copy, *wo_remote]

    row_seq = lax.rem(lax.broadcasted_iota(jnp.int32, (16, 128), 0), 8)
    q_copy.wait_recv()
    q_wide = [qh[h].astype(F32) for h in range(2)]

    def rows_of(i):
        return jnp.concatenate([q_wide[0][i * 8:i * 8 + 8], q_wide[1][i * 8:i * 8 + 8]], axis=0)

    def score(i):
        q_rows = rows_of(i)
        spread_q = jnp.concatenate([jnp.where(row_seq == b, q_rows, 0.0) for b in range(8)], axis=1).astype(BF16)
        for b in range(8):
            k_copies[i][b].wait()
            if i == 0:
                k_copies[1][b].start()
        for t in range(4):
            sbuf[:, t * 512:t * 512 + 512] = lax.dot_general(
                spread_q, kbuf[i, t * 512:t * 512 + 512], (((1,), (1,)), ((), ())), preferred_element_type=F32)

    def mix_values(i):
        new_k = nkv[0].astype(F32)[i * 8:i * 8 + 8]
        new_v = nkv[1].astype(F32)[i * 8:i * 8 + 8]
        new_k = jnp.concatenate([new_k, new_k], axis=0)
        new_v = jnp.concatenate([new_v, new_v], axis=0)
        score_new = jnp.sum(rows_of(i) * new_k, axis=1, keepdims=True) * SCALE
        row_len = jnp.zeros((16, 128), jnp.int32)
        for b in range(8):
            row_len = jnp.where(row_seq == b, len_ref[i * 8 + b], row_len)
        row_len = jnp.concatenate([row_len] * 16, axis=1)
        places = lax.broadcasted_iota(jnp.int32, (16, 2048), 1)
        scores = jnp.where(places < row_len, sbuf[...] * SCALE, -jnp.inf)
        top = jnp.maximum(jnp.max(scores, axis=1, keepdims=True), score_new)
        weights = jnp.exp(scores - top)
        weight_new = jnp.exp(score_new - top)
        denom = jnp.sum(weights, axis=1, keepdims=True) + weight_new
        weights = weights.astype(BF16)
        total = weight_new.astype(BF16).astype(F32) * new_v
        for b in range(8):
            v_copies[i][b].wait()
            if i == 0:
                v_copies[1][b].start()
        for c in range(4):
            both = jnp.dot(weights, vbuf[i, :, c * 256:c * 256 + 256], preferred_element_type=F32)
            total += jnp.where(row_seq == 2 * c, both[:, 0:128], 0.0) + jnp.where(row_seq == 2 * c + 1, both[:, 128:256], 0.0)
        obuf[i, core] = (total / denom).astype(BF16)
        return to_partner(obuf.at[i, core], obuf.at[i, core], o_s.at[i], o_v.at[i])

    rots = [jnp.where(core == 0, REDUCE_ROT[0][rg], REDUCE_ROT[1][rg]) for rg in range(4)]

    def project(i):
        pairs = [obuf[i, c].astype(F32) for c in range(2)]
        o = jnp.concatenate([jnp.concatenate([p[0:8], p[8:16]], axis=1) for p in pairs], axis=0).astype(BF16)

        @pl.loop(0, 16)
        def _(t):
            bz, by = lax.div(t, 4), lax.rem(t, 4)
            res = jnp.dot(o, wbuf[:, pl.ds(pl.multiple_of(t * 512, 512), 512)], preferred_element_type=F32)
            for bx in range(4):
                block = (bx, by, bz)
                for j, rg in enumerate(BATCH_GROUPS[i]):
                    at = pick(rots[rg], [block[d[0]] * 16 + block[d[1]] * 4 + block[d[2]] for d in ROTATIONS])
                    part[rg, at] = res[j * 8:j * 8 + 8, bx * 128:bx * 128 + 128]

    sources, widths, slots = (part, acc1, acc2), (16, 4, 1), (r1, r2, r3)
    send_sems, recv_sems = (s1, s2, s3), (v1, v2, v3)
    flying = {}

    def reduce_send(i, place):
        for rg in BATCH_GROUPS[i]:
            mine = coord_along(rots[rg], place, coord)
            copies = []
            for k in (2, 1, 3):
                there = lax.rem(mine + k, 4)
                copy = pltpu.make_async_remote_copy(
                    src_ref=sources[place].at[rg, pl.ds(there * widths[place], widths[place])],
                    dst_ref=slots[place].at[rg, k - 1],
                    send_sem=send_sems[place].at[rg, k - 1], recv_sem=recv_sems[place].at[rg, k - 1],
                    device_id={"heads": peer_along(rots[rg], place, coord, k), "model": core}, device_id_type=MESH)
                copy.start()
                copies.append(copy)
            flying[rg, place] = copies
            tail.extend(copies)

    def reduce_take(i, place):
        sums = []
        for rg in BATCH_GROUPS[i]:
            for copy in flying[rg, place]:
                copy.wait_recv()
            mine = coord_along(rots[rg], place, coord)
            got = slots[place]
            total = sources[place][rg, pl.ds(mine * widths[place], widths[place])] + got[rg, 0] + got[rg, 1] + got[rg, 2]
            if place < 2:
                sources[place + 1][rg] = total
            sums.append(total)
        return sums

    gather_rots = [jnp.where(core == 0, GATHER_ROT[0][i], GATHER_ROT[1][i]) for i in range(2)]
    gather_at = []
    for i in range(2):
        a, b, c = (coord_along(gather_rots[i], place, coord) for place in range(3))
        gather_at.append((c * 16 + b * 4 + a, c * 16 + b * 4, c * 16, c))
    gathering, crossing = {}, {0: [], 1: []}

    def gather_send(i, place):
        copies = {}
        for k in (2, 1, 3):
            ref = agbuf.at[core, i, pl.ds(gather_at[i][place], (1, 4, 16)[place])]
            copy = pltpu.make_async_remote_copy(
                src_ref=ref, dst_ref=ref, send_sem=ag_s.at[i, place, k - 1], recv_sem=ag_v.at[i, place, k - 1],
                device_id={"heads": peer_along(gather_rots[i], place, coord, k), "model": core}, device_id_type=MESH)
            copy.start()
            copies[k] = copy
        gathering[i, place] = copies
        tail.extend(copies.values())

    def gather_wait(i, place):
        for copy in gathering[i, place].values():
            copy.wait_recv()

    def cross(i, k):
        ref = agbuf.at[core, i, pl.ds(lax.rem(gather_at[i][3] + 4 - k, 4) * 16, 16)]
        copy = to_partner(ref, ref, dd_s.at[i, k], dd_v.at[i, k])
        crossing[i].append(copy)
        tail.append(copy)

    token_col = pl.multiple_of(core * HALF + chip * 128, 128)

    def finish(i):
        sums = reduce_take(i, 2)
        own = tok[:, pl.ds(token_col, 128)].astype(F32)
        rows = [own[rg * 8:rg * 8 + 8] + sums[j][0] for j, rg in enumerate(BATCH_GROUPS[i])]
        agbuf[core, i, gather_at[i][0]] = jnp.concatenate(rows, axis=0).astype(BF16)
        gather_send(i, 0)

    score(0)
    n_copy.wait_recv()
    kg[group] = nkv[...]
    new_copies = []
    for n, (dy, dz) in enumerate(((0, 1), (0, 2), (0, 3), (2, 0), (2, 1), (2, 2), (2, 3))):
        copy = pltpu.make_async_remote_copy(
            src_ref=nkv, dst_ref=kg.at[group], send_sem=g_s.at[n], recv_sem=g_v.at[n],
            device_id={"heads": chip_of(moved(moved(coord, 1, dy), 2, dz)), "model": core}, device_id_type=MESH)
        copy.start()
        new_copies.append(copy)
    tail += new_copies
    o_copy = mix_values(0)
    tail.append(o_copy)
    score(1)
    wo_copy.wait()
    for copy in wo_remote:
        copy.wait_recv()
    o_copy.wait_recv()
    project(0)
    reduce_send(0, 0)
    o_copy = mix_values(1)
    tail.append(o_copy)
    o_copy.wait_recv()
    project(1)
    reduce_send(1, 0)
    reduce_take(0, 0)
    reduce_send(0, 1)
    reduce_take(1, 0)
    reduce_send(1, 1)
    reduce_take(0, 1)
    reduce_send(0, 2)
    reduce_take(1, 1)
    reduce_send(1, 2)
    finish(0)
    finish(1)
    for place in range(2):
        for i in range(2):
            gather_wait(i, place)
            gather_send(i, place + 1)
            if place == 1:
                cross(i, 0)
    for copy in new_copies:
        copy.wait_recv()
    new_ref[...] = kg[...]
    for k in (1, 3, 2):
        for i in range(2):
            gathering[i, 2][k].wait_recv()
            cross(i, k)
    for i in range(2):
        for copy in crossing[i]:
            copy.wait_recv()
    for cc in range(2):
        for bz in range(4):
            for by in range(4):
                for bx in range(4):
                    b = (bx, by, bz)
                    tiles = []
                    for i in range(2):
                        dims = ROTATIONS[GATHER_ROT[cc][i]]
                        tiles.append(agbuf[cc, i, b[dims[2]] * 16 + b[dims[1]] * 4 + b[dims[0]]].astype(F32))
                    col = cc * HALF + chip_of(b) * 128
                    for j in range(2):
                        out_ref[j * 16:j * 16 + 16, col:col + 128] = jnp.concatenate(
                            [tiles[0][j * 8:j * 8 + 8], tiles[1][j * 8:j * 8 + 8]], axis=0).astype(BF16)
    for copy in tail:
        copy.wait_send()


def step(tokens, w_query, w_key, w_value, w_out, key_cache, value_cache, lengths):
    dma = pltpu.SemaphoreType.DMA
    vmem = pltpu.VMEM
    out, new = pl.pallas_call(
        step_kernel,
        out_shape=(jax.ShapeDtypeStruct((32, 16384), BF16), jax.ShapeDtypeStruct((8, 2, 16, 128), BF16)),
        in_specs=[pl.BlockSpec(memory_space=pltpu.SMEM)] + [pl.BlockSpec(memory_space=pl.ANY)] * 7,
        out_specs=(pl.BlockSpec(memory_space=pltpu.VMEM),) * 2,
        scratch_shapes=[
            vmem((32, 16384), BF16), vmem((8, 2048, 128), BF16), vmem((8, 2048, 128), BF16),
            vmem((2, 2048, 1024), BF16), vmem((2, 2048, 1024), BF16), vmem((256, HALF), BF16),
            vmem((2, 16, 128), BF16), vmem((2, 16, 128), BF16), vmem((2, 16, 128), BF16), vmem((2, 16, 128), BF16),
            vmem((8, 2, 16, 128), BF16), vmem((2, 2, 16, 128), BF16), vmem((16, 2048), F32),
            vmem((4, 64, 8, 128), F32), vmem((4, 3, 16, 8, 128), F32),
            vmem((4, 16, 8, 128), F32), vmem((4, 3, 4, 8, 128), F32), vmem((4, 4, 8, 128), F32),
            vmem((4, 3, 1, 8, 128), F32), vmem((2, 2, 64, 16, 128), BF16),
            dma, dma((8,)), dma((8,)), dma((2, 8)), dma((2, 8)), dma, dma((2,)), dma((2,)),
            dma, dma, dma, dma, dma((7,)), dma((7,)), dma((2,)), dma((2,)),
            dma((4, 3)), dma((4, 3)), dma((4, 3)), dma((4, 3)), dma((4, 3)), dma((4, 3)),
            dma((2, 3, 3)), dma((2, 3, 3)), dma((2, 4)), dma((2, 4)),
        ],
        compiler_params=pltpu.CompilerParams(collective_id=0, has_side_effects=True, vmem_limit_bytes=60000 * 1024),
    )(lengths, tokens, w_query, w_key, w_value, w_out, key_cache, value_cache)
    return out, new[:, 0].transpose(1, 0, 2), new[:, 1].transpose(1, 0, 2)


def solution(mesh):
    cache_spec = P(("replica", "model"), None, None, None)
    new_spec = P(("replica", "model"), None, None)
    return jax.shard_map(
        step,
        mesh=mesh,
        in_specs=(P("replica", None), P(None, ("heads", "model")), P(None, None), P(None, None), P(("heads", "model"), None), cache_spec, cache_spec, P(("replica", "model"))),
        out_specs=(P("replica", None), new_spec, new_spec),
        check_vma=False,
    )
```
